32 devices in a mesh: section: 2 (over x), outer: 4 (over y, core), tensor: 4 (over z).
Axes of the slice: x: 2, y: 2, z: 4, core: 2. Of those that a mesh axis runs over, the one named last changes fastest.
Arguments:
- act_in: bfloat16 [2, 16, 8192], P('section', 'outer', 'tensor'), may hold values from -6 to 6
- saved_in: bfloat16 [2, 16, 8192], P('section', 'outer', 'tensor'), may hold values from -6 to 6
- cotangent: bfloat16 [2, 16, 8192], P('section', 'outer', 'tensor'), may hold values from -6 to 6
- w_gate: bfloat16 [2, 8192, 14336], P('section', 'tensor', 'outer'), may hold values from -0.0625 to 0.0625
- w_up: bfloat16 [2, 8192, 14336], P('section', 'tensor', 'outer'), may hold values from -0.0625 to 0.0625
- w_down: bfloat16 [2, 14336, 8192], P('section', 'outer', 'tensor'), may hold values from -0.046875 to 0.046875
Outputs:
- forward_sent: bfloat16 [2, 16, 8192], P('section', 'outer', 'tensor')
- grad_sent: bfloat16 [2, 16, 8192], P('section', 'outer', 'tensor')
The draws below stay inside these ranges and needn't reach their ends.
All inputs are finite; a program needn't handle non-finite values.
Results may differ from the reference program's by a relative error of at most 0.025.
Values may be sent and summed in bfloat16 or wider, within the bound.
A program may use at most 128 MiB of HBM per device.

```python
import jax
import jax.numpy as jnp
from jax import lax

D = 8192
H = 14336
CELL_ROWS = 1
GROUPS = 4
TOKENS = 16
D_BLOCK = 2048
N_TENSOR = 4


def levels(rng, extent, cuts, least, largest):
    factor_of = 1.0
    for axis_at, blocks in cuts:
        draws = jax.random.uniform(jax.random.fold_in(jax.random.fold_in(rng, 6), axis_at), (blocks,), jnp.float32, least / len(cuts), largest / len(cuts))
        factor_of = factor_of * jnp.repeat(jnp.exp(draws), extent[axis_at] // blocks).reshape((-1,) + (1,) * (len(extent) - 1 - axis_at))
    return factor_of


def bell_draw(stream_key, shape, width, reach, cuts=(), kind=jnp.bfloat16):
    gain = levels(stream_key, shape, cuts, -0.22, 0.18) if cuts else 1.0
    drawn = jax.random.normal(stream_key, shape, jnp.float32) * width * gain
    return jnp.minimum(jnp.maximum(drawn, -reach), reach).astype(kind)


def setup_inputs(seed: int = 0) -> dict:
    arg_keys = jax.random.split(jax.random.key(seed), 7)
    act_in = bell_draw(arg_keys[0], (2, TOKENS, D), 1.0, 6.0, ((0, 2), (1, 4), (2, 4)))
    saved_in = bell_draw(arg_keys[1], (2, TOKENS, D), 1.0, 6.0, ((0, 2), (1, 4), (2, 4)))
    cotangent = bell_draw(arg_keys[2], (2, TOKENS, D), 1.0, 6.0, ((0, 2), (1, 4), (2, 4)))
    w_gate = bell_draw(arg_keys[3], (2, D, H), D ** -0.5, 0.0625, ((0, 2), (1, 4), (2, 4)))
    w_up = bell_draw(arg_keys[4], (2, D, H), D ** -0.5, 0.0625, ((0, 2), (1, 4), (2, 4)))
    w_down = bell_draw(arg_keys[5], (2, H, D), H ** -0.5, 0.046875, ((0, 2), (1, 4), (2, 4)))
    return dict(act_in=act_in, saved_in=saved_in, cotangent=cotangent, w_gate=w_gate, w_up=w_up, w_down=w_down)


def reorder(matrix):
    return matrix.reshape(GROUPS, GROUPS, CELL_ROWS, matrix.shape[1]).transpose(1, 0, 2, 3).reshape(matrix.shape)


def rounded(product):
    return lax.optimization_barrier(product.astype(jnp.bfloat16)).astype(jnp.float32)


def block_sum(left, right):
    left_blocks = left.reshape(TOKENS, N_TENSOR, D_BLOCK).transpose(1, 0, 2)
    right_blocks = right.reshape(N_TENSOR, D_BLOCK, right.shape[1])

    def add_block(running, pieces):
        partial_value = jnp.dot(pieces[0], pieces[1], preferred_element_type=jnp.float32)
        return running + rounded(partial_value), None

    begin_sum = jnp.zeros((TOKENS, right.shape[1]), jnp.float32)
    result, unused = lax.scan(add_block, begin_sum, (left_blocks, right_blocks))
    return result


def section_math(current, stored, incoming, gate_mat, up_mat, down_mat):
    gate_pre = block_sum(current, gate_mat)
    up_pre = block_sum(current, up_mat)
    hidden = (jax.nn.silu(gate_pre) * up_pre).astype(jnp.bfloat16)
    output = (current.astype(jnp.float32) + jnp.dot(hidden, down_mat, preferred_element_type=jnp.float32)).astype(jnp.bfloat16)
    gate_saved = block_sum(stored, gate_mat)
    up_saved = block_sum(stored, up_mat)
    hidden_grad = block_sum(incoming, down_mat.T)
    squash = jax.nn.sigmoid(gate_saved)
    gate_grad = (hidden_grad * up_saved * squash * (1.0 + gate_saved * (1.0 - squash))).astype(jnp.bfloat16)
    up_grad = (hidden_grad * gate_saved * squash).astype(jnp.bfloat16)
    backward = jnp.dot(gate_grad, gate_mat.T, preferred_element_type=jnp.float32) + jnp.dot(up_grad, up_mat.T, preferred_element_type=jnp.float32)
    input_grad = (incoming.astype(jnp.float32) + backward).astype(jnp.bfloat16)
    return output, input_grad


def reference(act_in, saved_in, cotangent, w_gate, w_up, w_down):
    first = section_math(act_in[0], saved_in[0], cotangent[0], w_gate[0], w_up[0], w_down[0])
    second = section_math(act_in[1], saved_in[1], cotangent[1], w_gate[1], w_up[1], w_down[1])
    forward_sent = jnp.stack([reorder(second[0]), reorder(first[0])])
    grad_sent = jnp.stack([reorder(second[1]), reorder(first[1])])
    return forward_sent, grad_sent
```

```python
import functools

import jax
import jax.numpy as jnp
from jax import lax
from jax.experimental import pallas as pl
from jax.experimental.pallas import tpu as pltpu
from jax.sharding import PartitionSpec as P

MESH = pl.DeviceIdType.MESH
F32 = jnp.float32
BF16 = jnp.bfloat16
CONTRACT_LAST = (((1,), (1,)), ((), ()))
SUM_LAG = 2
SECOND_LAG = 4
AHEAD = 2
SUM_AFTER = 3
SECOND_AFTER = 5
PAIRED = 0


def kernel(
    sections, outers, tensors, chunks, chunk,
    act, saved, cot, w_gate, w_up, w_down,
    out_ref, grad_ref,
    gate_buf, up_buf, down_buf, gathered, staging, rows_f32, lhs_two, lhs_cot,
    products, part, arrived, shared, second_f32, total, final_out, final_in,
    load_sem, weight_sem, gather_send, gather_recv, part_send, part_recv,
    share_send, share_recv, final_send, final_recv,
):
    section = lax.axis_index("section")
    outer = lax.axis_index("outer")
    tensor = lax.axis_index("tensor")
    other = lax.rem(section + 1, sections)
    own_rows = act.shape[1]
    rows = own_rows * outers
    cells = own_rows // outers
    shard = rows // tensors

    loads = [
        pltpu.make_async_copy(source.at[0], gathered.at[which, outer], load_sem.at[which])
        for which, source in enumerate((act, saved, cot))
    ]
    for load in loads:
        load.start()

    def weight_copies(c):
        span = pl.ds(pl.multiple_of(c * chunk, chunk), chunk)
        return (
            pltpu.make_async_copy(w_gate.at[0, :, span], gate_buf.at[c], weight_sem.at[0, c]),
            pltpu.make_async_copy(w_up.at[0, :, span], up_buf.at[c], weight_sem.at[1, c]),
            pltpu.make_async_copy(w_down.at[0, span, :], down_buf.at[c], weight_sem.at[2, c]),
        )

    for c in range(min(AHEAD, chunks)):
        for copy in weight_copies(c):
            copy.start(priority=1)

    barrier = pltpu.get_barrier_semaphore()
    for step in range(1, outers):
        pl.semaphore_signal(
            barrier, 1, device_id={"outer": lax.rem(outer + step, outers)}, device_id_type=MESH
        )
    for step in range(1, tensors):
        pl.semaphore_signal(
            barrier, 1, device_id={"tensor": lax.rem(tensor + step, tensors)}, device_id_type=MESH
        )
    for place in range(outers):
        pl.semaphore_signal(
            barrier, 1, device_id={"section": other, "outer": place}, device_id_type=MESH
        )
    pl.semaphore_wait(barrier, 2 * outers + tensors - 2)

    def gather_copy(which, origin, target):
        return pltpu.make_async_remote_copy(
            src_ref=gathered.at[which, origin],
            dst_ref=gathered.at[which, origin],
            send_sem=gather_send.at[which, target],
            recv_sem=gather_recv.at[which, origin],
            device_id={"outer": target},
            device_id_type=MESH,
        )

    for which in range(3):
        loads[which].wait()
        for step in range(1, outers):
            gather_copy(which, outer, lax.rem(outer + step, outers)).start()

    for which in range(3):
        for step in range(1, outers):
            origin = lax.rem(outer + step, outers)
            gather_copy(which, origin, origin).wait_recv()
        for origin in range(outers):
            staging[...] = gathered[which, origin].astype(F32)
            for j in range(outers):
                to = (j * outers + origin) * cells
                rows_f32[which, to : to + cells, :] = staging[j * cells : (j + 1) * cells, :]
    lhs_two[0:rows, :] = rows_f32[0].astype(BF16)
    lhs_two[rows : 2 * rows, :] = rows_f32[1].astype(BF16)
    lhs_cot[...] = rows_f32[2].astype(BF16)
    place = lax.broadcasted_iota(jnp.int32, total.shape[1:], 0)
    mine = lax.rem(lax.div(place, cells), outers) == outer
    total[0] = jnp.where(mine, rows_f32[0], 0.0)
    total[1] = jnp.where(mine, rows_f32[2], 0.0)

    def part_copy(c, origin, target):
        return pltpu.make_async_remote_copy(
            src_ref=part.at[c, target],
            dst_ref=arrived.at[c, origin],
            send_sem=part_send.at[c, target],
            recv_sem=part_recv.at[c, origin],
            device_id={"tensor": target},
            device_id_type=MESH,
        )

    def share_copy(c, origin, target):
        return pltpu.make_async_remote_copy(
            src_ref=shared.at[c, origin],
            dst_ref=shared.at[c, origin],
            send_sem=share_send.at[c, target],
            recv_sem=share_recv.at[c, origin],
            device_id={"tensor": target},
            device_id_type=MESH,
        )

    def first(c):
        @pl.when(c + AHEAD < chunks)
        def _():
            for copy in weight_copies(c + AHEAD):
                copy.start(priority=1)

        for copy in weight_copies(c):
            copy.wait()
        two = lhs_two[...]
        products[0 : 2 * rows, :] = jnp.dot(two, gate_buf[c], preferred_element_type=F32)
        products[2 * rows : 4 * rows, :] = jnp.dot(two, up_buf[c], preferred_element_type=F32)
        products[4 * rows : 5 * rows, :] = lax.dot_general(
            lhs_cot[...], down_buf[c], CONTRACT_LAST, preferred_element_type=F32
        )
        for target in range(tensors):
            for which in range(5):
                part[c, target, which] = products[
                    which * rows + target * shard : which * rows + (target + 1) * shard, :
                ].astype(BF16)
        for step in range(1, tensors):
            part_copy(c, tensor, lax.rem(tensor + step, tensors)).start()

    def combine(c):
        for step in range(1, tensors):
            origin = lax.rem(tensor + step, tensors)
            part_copy(c, origin, origin).wait_recv()
        sums = []
        for which in range(5):
            summed = part[c, tensor, which].astype(F32)
            for step in range(1, tensors):
                summed = summed + arrived[c, lax.rem(tensor + step, tensors), which].astype(F32)
            sums.append(summed)
        gate_pre, gate_saved, up_pre, up_saved, hidden_grad = sums
        squash = jax.nn.sigmoid(gate_saved)
        shared[c, tensor, 0] = (gate_pre * jax.nn.sigmoid(gate_pre) * up_pre).astype(BF16)
        shared[c, tensor, 1] = (
            hidden_grad * up_saved * squash * (1.0 + gate_saved * (1.0 - squash))
        ).astype(BF16)
        shared[c, tensor, 2] = (hidden_grad * gate_saved * squash).astype(BF16)
        for step in range(1, tensors):
            share_copy(c, tensor, lax.rem(tensor + step, tensors)).start()

    def second(c):
        for step in range(1, tensors):
            origin = lax.rem(tensor + step, tensors)
            share_copy(c, origin, origin).wait_recv()
        for origin in range(tensors):
            for which in range(3):
                second_f32[which, origin * shard : (origin + 1) * shard, :] = shared[
                    c, origin, which
                ].astype(F32)
        total[0] += jnp.dot(
            second_f32[0].astype(BF16), down_buf[c], preferred_element_type=F32
        )
        total[1] += lax.dot_general(
            second_f32[1].astype(BF16), gate_buf[c], CONTRACT_LAST, preferred_element_type=F32
        ) + lax.dot_general(
            second_f32[2].astype(BF16), up_buf[c], CONTRACT_LAST, preferred_element_type=F32
        )

    def advance(step, carry):
        @pl.when(step < chunks)
        def _():
            first(step)

        @pl.when((step >= SUM_LAG) & (step < chunks + SUM_LAG))
        def _():
            combine(step - SUM_LAG)

        @pl.when(step >= SECOND_LAG)
        def _():
            second(step - SECOND_LAG)

        return carry

    lax.fori_loop(0, chunks + SECOND_LAG, advance, 0)

    def final_copy(origin, target):
        return pltpu.make_async_remote_copy(
            src_ref=final_out.at[target],
            dst_ref=final_in.at[origin],
            send_sem=final_send.at[target],
            recv_sem=final_recv.at[origin],
            device_id={"section": other, "outer": target},
            device_id_type=MESH,
        )

    for target in range(outers):
        for which in range(2):
            final_out[target, which] = total[
                which, target * own_rows : (target + 1) * own_rows, :
            ].astype(BF16)
        final_copy(outer, target).start()

    def drain(c, carry):
        for step in range(1, tensors):
            target = lax.rem(tensor + step, tensors)
            part_copy(c, tensor, target).wait_send()
            share_copy(c, tensor, target).wait_send()
        return carry

    lax.fori_loop(0, chunks, drain, 0)
    for which in range(3):
        for step in range(1, outers):
            gather_copy(which, outer, lax.rem(outer + step, outers)).wait_send()

    for origin in range(outers):
        final_copy(origin, origin).wait_recv()
    for which, result in enumerate((out_ref, grad_ref)):
        summed = final_in[0, which].astype(F32)
        for origin in range(1, outers):
            summed = summed + final_in[origin, which].astype(F32)
        result[0] = summed.astype(BF16)
    for target in range(outers):
        final_copy(outer, target).wait_send()


def fast_kernel(
    outers, tensors, chunks, chunk, paired,
    act, saved, cot, w_gate, w_up, w_down,
    out_ref,
    gate_buf, up_buf, down_buf, up_turned, gathered, rows_f32, lhs_two, lhs_cot,
    part, arrived, passed, joined, shared, total, final_out, final_in,
    load_sem, weight_sem, gather_send, gather_recv, part_send, part_recv, pass_recv,
    share_send, share_recv, final_send, final_recv,
):
    section = lax.axis_index("section")
    outer = lax.axis_index("outer")
    tensor = lax.axis_index("tensor")
    other = 1 - section
    own_rows = act.shape[1]
    rows = own_rows * outers
    lanes = chunk // tensors
    left = tensor < 2
    is_end = (tensor == 0) | (tensor == 3)
    partner = tensor + 1 - 2 * lax.rem(tensor, 2)
    far_inner = jnp.where(left, 2, 1)
    far_end = jnp.where(left, 3, 0)
    fars = (far_inner, far_end)
    peers = [lax.rem(tensor + step, tensors) for step in range(1, tensors)]

    loads = [
        pltpu.make_async_copy(source.at[0], gathered.at[which, outer], load_sem.at[which])
        for which, source in enumerate((act, saved, cot))
    ]
    for load in loads:
        load.start()
    weight_copies = []
    for c in range(chunks):
        span = pl.ds(c * chunk, chunk)
        copies = (
            pltpu.make_async_copy(w_gate.at[0, :, span], gate_buf.at[c], weight_sem.at[0, c]),
            pltpu.make_async_copy(w_up.at[0, :, span], up_buf.at[c], weight_sem.at[1, c]),
            pltpu.make_async_copy(w_down.at[0, span, :], down_buf.at[c], weight_sem.at[2, c]),
        )
        for copy in copies:
            copy.start(priority=1)
        weight_copies.append(copies)

    barrier = pltpu.get_barrier_semaphore()
    for step in range(1, outers):
        pl.semaphore_signal(
            barrier, 1, device_id={"outer": lax.rem(outer + step, outers)}, device_id_type=MESH
        )
    for peer in peers:
        pl.semaphore_signal(barrier, 1, device_id={"tensor": peer}, device_id_type=MESH)
    for place in range(outers):
        pl.semaphore_signal(
            barrier, 1, device_id={"section": other, "outer": place}, device_id_type=MESH
        )
    for load in loads:
        load.wait()
    pl.semaphore_wait(barrier, 2 * outers + tensors - 2)

    def gather_copy(which, origin, target):
        return pltpu.make_async_remote_copy(
            src_ref=gathered.at[which, origin],
            dst_ref=gathered.at[which, origin],
            send_sem=gather_send.at[which, target],
            recv_sem=gather_recv.at[which, origin],
            device_id={"outer": target},
            device_id_type=MESH,
        )

    for which in range(3):
        for step in range(1, outers):
            gather_copy(which, outer, lax.rem(outer + step, outers)).start()
    for which in range(3):
        for step in range(1, outers):
            origin = lax.rem(outer + step, outers)
            gather_copy(which, origin, origin).wait_recv()
        for origin in range(outers):
            rows_f32[which, origin * own_rows : (origin + 1) * own_rows, :] = gathered[
                which, origin
            ].astype(F32)
    row = lax.broadcasted_iota(jnp.int32, (rows, rows), 0)
    column = lax.broadcasted_iota(jnp.int32, (rows, rows), 1)
    takes = lax.rem(row, outers) * own_rows + lax.div(row, outers) == column
    turn = jnp.where(takes, 1.0, 0.0).astype(BF16)
    ordered = [
        jnp.dot(turn, rows_f32[which].astype(BF16), preferred_element_type=F32)
        for which in range(3)
    ]
    lhs_two[0:rows, :] = ordered[0].astype(BF16)
    lhs_two[rows : 2 * rows, :] = ordered[1].astype(BF16)
    lhs_cot[...] = ordered[2].astype(BF16)
    place = lax.broadcasted_iota(jnp.int32, total.shape[1:], 0)
    mine = lax.rem(place, outers) == outer
    total[0] = jnp.where(mine, ordered[0], 0.0)
    total[1] = jnp.where(mine, ordered[2], 0.0)

    def part_copy(c, source, origin, target):
        return pltpu.make_async_remote_copy(
            src_ref=source,
            dst_ref=arrived.at[c, origin],
            send_sem=part_send.at[c, target],
            recv_sem=part_recv.at[c, origin],
            device_id={"tensor": target},
            device_id_type=MESH,
        )

    def pass_copy(c, k, far):
        return pltpu.make_async_remote_copy(
            src_ref=part.at[c, far],
            dst_ref=passed.at[c, k],
            send_sem=part_send.at[c, far],
            recv_sem=pass_recv.at[c, k],
            device_id={"tensor": partner},
            device_id_type=MESH,
        )

    def share_copy(c, origin, target):
        return pltpu.make_async_remote_copy(
            src_ref=shared.at[c, origin],
            dst_ref=shared.at[c, origin],
            send_sem=share_send.at[c, target],
            recv_sem=share_recv.at[c, origin],
            device_id={"tensor": target},
            device_id_type=MESH,
        )

    def first(c):
        for copy in weight_copies[c]:
            copy.wait()
        gate = jnp.dot(lhs_two[...], gate_buf[c], preferred_element_type=F32)
        up = jnp.dot(lhs_two[...], up_buf[c], preferred_element_type=F32)
        grad = lax.dot_general(lhs_cot[...], down_buf[c], CONTRACT_LAST, preferred_element_type=F32)
        for target in range(tensors):
            span = slice(target * lanes, (target + 1) * lanes)
            part[c, target, 0 : 2 * rows] = gate[:, span].astype(BF16)
            part[c, target, 2 * rows : 4 * rows] = up[:, span].astype(BF16)
            part[c, target, 4 * rows : 5 * rows] = grad[:, span].astype(BF16)
        if c < paired:
            @pl.when(is_end)
            def _():
                for k, far in enumerate(fars):
                    pass_copy(c, k, far).start()

            part_copy(c, part.at[c, partner], tensor, partner).start()
        else:
            for peer in peers:
                part_copy(c, part.at[c, peer], tensor, peer).start()
        up_turned[c] = up_buf[c].T

    def relay(c):
        if c >= paired:
            return

        @pl.when(jnp.logical_not(is_end))
        def _():
            for k, far in enumerate(fars):
                pass_copy(c, k, far).wait_recv()
                joined[c, k] = (part[c, far].astype(F32) + passed[c, k].astype(F32)).astype(BF16)
                part_copy(c, joined.at[c, k], tensor, far).start()

    def combine(c):
        origins = [partner, far_inner] if c < paired else peers
        for origin in origins:
            part_copy(c, part.at[c, origin], origin, origin).wait_recv()
        summed = part[c, tensor].astype(F32)
        for origin in origins:
            summed = summed + arrived[c, origin].astype(F32)
        gate_pre, gate_saved, up_pre, up_saved, hidden_grad = (
            summed[which * rows : (which + 1) * rows] for which in range(5)
        )
        squash = jax.nn.sigmoid(gate_saved)
        shared[c, tensor, 0:rows] = (gate_pre * jax.nn.sigmoid(gate_pre) * up_pre).astype(BF16)
        shared[c, tensor, rows : 2 * rows] = (
            hidden_grad * up_saved * squash * (1.0 + gate_saved * (1.0 - squash))
        ).astype(BF16)
        shared[c, tensor, 2 * rows : 3 * rows] = (hidden_grad * gate_saved * squash).astype(BF16)
        for peer in peers:
            share_copy(c, tensor, peer).start()

    def final_copy(which, origin, target):
        return pltpu.make_async_remote_copy(
            src_ref=final_out.at[which, target],
            dst_ref=final_in.at[which, origin],
            send_sem=final_send.at[which, target],
            recv_sem=final_recv.at[which, origin],
            device_id={"section": other, "outer": target},
            device_id_type=MESH,
        )

    def send_final(which):
        for target in range(outers):
            final_out[which, target] = total[
                which, target * own_rows : (target + 1) * own_rows, :
            ].astype(BF16)
            final_copy(which, outer, target).start()

    def second(c):
        for peer in peers:
            share_copy(c, peer, peer).wait_recv()

        def side(which):
            return jnp.concatenate(
                [shared[c, t, which * rows : (which + 1) * rows] for t in range(tensors)], axis=1
            )

        total[0] += jnp.dot(side(0), down_buf[c], preferred_element_type=F32)
        if c == chunks - 1:
            send_final(0)
        total[1] += lax.dot_general(
            side(1), gate_buf[c], CONTRACT_LAST, preferred_element_type=F32
        ) + jnp.dot(side(2), up_turned[c], preferred_element_type=F32)

    last = chunks - 1
    for step in range(chunks):
        first(step)
        if step >= 1:
            relay(step - 1)
        if step >= SUM_AFTER:
            combine(step - SUM_AFTER)
        if step >= SECOND_AFTER:
            second(step - SECOND_AFTER)
    done = max(chunks - SECOND_AFTER, 0)
    for c in range(max(chunks - SUM_AFTER, 0), chunks):
        combine(c) if c < last else relay(c)
        if c < last and done < c:
            second(done)
            done += 1
    combine(last)
    while done < chunks:
        second(done)
        done += 1
    send_final(1)

    def drain(c, carry):
        for peer in peers:
            part_copy(c, part.at[c, peer], tensor, peer).wait_send()
            share_copy(c, tensor, peer).wait_send()
        return carry

    lax.fori_loop(0, chunks, drain, 0)
    for which in range(3):
        for step in range(1, outers):
            gather_copy(which, outer, lax.rem(outer + step, outers)).wait_send()
    for which in range(2):
        for origin in range(outers):
            final_copy(which, origin, origin).wait_recv()
        summed = final_in[which, 0].astype(F32)
        for origin in range(1, outers):
            summed = summed + final_in[which, origin].astype(F32)
        out_ref[which] = summed.astype(BF16)
    for which in range(2):
        for target in range(outers):
            final_copy(which, outer, target).wait_send()


def part_out(both, out_ref, grad_ref):
    out_ref[0] = both[0]
    grad_ref[0] = both[1]


def fast_call(outers, tensors, chunk, act_in, saved_in, cotangent, w_gate, w_up, w_down):
    own_rows, model_width = act_in.shape[1:]
    chunks = w_gate.shape[2] // chunk
    rows = own_rows * outers
    lanes = chunk // tensors
    dma = pltpu.SemaphoreType.DMA
    both = pl.pallas_call(
        functools.partial(fast_kernel, outers, tensors, chunks, chunk, PAIRED),
        out_shape=jax.ShapeDtypeStruct((2, own_rows, model_width), BF16),
        in_specs=[pl.BlockSpec(memory_space=pl.ANY)] * 6,
        out_specs=pl.BlockSpec(memory_space=pltpu.VMEM),
        scratch_shapes=[
            pltpu.VMEM((chunks, model_width, chunk), BF16),
            pltpu.VMEM((chunks, model_width, chunk), BF16),
            pltpu.VMEM((chunks, chunk, model_width), BF16),
            pltpu.VMEM((chunks, chunk, model_width), BF16),
            pltpu.VMEM((3, outers, own_rows, model_width), BF16),
            pltpu.VMEM((3, rows, model_width), F32),
            pltpu.VMEM((2 * rows, model_width), BF16),
            pltpu.VMEM((rows, model_width), BF16),
            pltpu.VMEM((chunks, tensors, 5 * rows, lanes), BF16),
            pltpu.VMEM((chunks, tensors, 5 * rows, lanes), BF16),
            pltpu.VMEM((chunks, 2, 5 * rows, lanes), BF16),
            pltpu.VMEM((chunks, 2, 5 * rows, lanes), BF16),
            pltpu.VMEM((chunks, tensors, 3 * rows, lanes), BF16),
            pltpu.VMEM((2, rows, model_width), F32),
            pltpu.VMEM((2, outers, own_rows, model_width), BF16),
            pltpu.VMEM((2, outers, own_rows, model_width), BF16),
            dma((3,)),
            dma((3, chunks)),
            dma((3, outers)),
            dma((3, outers)),
            dma((chunks, tensors)),
            dma((chunks, tensors)),
            dma((chunks, 2)),
            dma((chunks, tensors)),
            dma((chunks, tensors)),
            dma((2, outers)),
            dma((2, outers)),
        ],
        compiler_params=pltpu.CompilerParams(
            collective_id=0, has_side_effects=True, vmem_limit_bytes=63 * 1024 * 1024
        ),
    )(act_in, saved_in, cotangent, w_gate, w_up, w_down)
    out = jax.ShapeDtypeStruct((1, own_rows, model_width), BF16)
    return pl.pallas_call(part_out, out_shape=(out, out))(both)


def solution(mesh):
    sections, outers, tensors = (mesh.shape[name] for name in ("section", "outer", "tensor"))

    def on_device(act_in, saved_in, cotangent, w_gate, w_up, w_down):
        own_rows, model_width = act_in.shape[1:]
        width = w_gate.shape[2]
        rows = own_rows * outers
        if sections == 2 and tensors == 4 and own_rows == outers and rows % 16 == 0 and width % 512 == 0:
            if 4 * width * model_width * 2 <= 56 * 1024 * 1024:
                return fast_call(
                    outers, tensors, 512, act_in, saved_in, cotangent, w_gate, w_up, w_down
                )
        shard = rows // tensors
        chunk = next(size for size in (512, 256, 128, width) if width % size == 0)
        chunks = width // chunk
        dma = pltpu.SemaphoreType.DMA
        out = jax.ShapeDtypeStruct((1, own_rows, model_width), BF16)
        return pl.pallas_call(
            functools.partial(kernel, sections, outers, tensors, chunks, chunk),
            out_shape=(out, out),
            in_specs=[pl.BlockSpec(memory_space=pl.ANY)] * 6,
            out_specs=[pl.BlockSpec(memory_space=pltpu.VMEM)] * 2,
            scratch_shapes=[
                pltpu.VMEM((chunks, model_width, chunk), BF16),
                pltpu.VMEM((chunks, model_width, chunk), BF16),
                pltpu.VMEM((chunks, chunk, model_width), BF16),
                pltpu.VMEM((3, outers, own_rows, model_width), BF16),
                pltpu.VMEM((own_rows, model_width), F32),
                pltpu.VMEM((3, rows, model_width), F32),
                pltpu.VMEM((2 * rows, model_width), BF16),
                pltpu.VMEM((rows, model_width), BF16),
                pltpu.VMEM((5 * rows, chunk), F32),
                pltpu.VMEM((chunks, tensors, 5, shard, chunk), BF16),
                pltpu.VMEM((chunks, tensors, 5, shard, chunk), BF16),
                pltpu.VMEM((chunks, tensors, 3, shard, chunk), BF16),
                pltpu.VMEM((3, rows, chunk), F32),
                pltpu.VMEM((2, rows, model_width), F32),
                pltpu.VMEM((outers, 2, own_rows, model_width), BF16),
                pltpu.VMEM((outers, 2, own_rows, model_width), BF16),
                dma((3,)),
                dma((3, chunks)),
                dma((3, outers)),
                dma((3, outers)),
                dma((chunks, tensors)),
                dma((chunks, tensors)),
                dma((chunks, tensors)),
                dma((chunks, tensors)),
                dma((outers,)),
                dma((outers,)),
            ],
            compiler_params=pltpu.CompilerParams(
                collective_id=0, has_side_effects=True, vmem_limit_bytes=60 * 1024 * 1024
            ),
        )(act_in, saved_in, cotangent, w_gate, w_up, w_down)

    return jax.shard_map(
        on_device,
        mesh=mesh,
        in_specs=(
            P("section", "outer", "tensor"),
            P("section", "outer", "tensor"),
            P("section", "outer", "tensor"),
            P("section", "tensor", "outer"),
            P("section", "tensor", "outer"),
            P("section", "outer", "tensor"),
        ),
        out_specs=(P("section", "outer", "tensor"), P("section", "outer", "tensor")),
        check_vma=False,
    )
```

```python
import functools

import jax
import jax.numpy as jnp
from jax import lax
from jax.experimental import pallas as pl
from jax.experimental.pallas import tpu as pltpu
from jax.sharding import PartitionSpec as P

MESH = pl.DeviceIdType.MESH
F32 = jnp.float32
BF16 = jnp.bfloat16
CONTRACT_LAST = (((1,), (1,)), ((), ()))
SUM_LAG = 2
SECOND_LAG = 4
AHEAD = 2
RELAY_AFTER = 2
SUM_AFTER = 4
DIRECT_AFTER = 3
SECOND_AFTER = 6
DIRECT_FIRST = 2
DIRECT_LAST = 0


def kernel(
    sections, outers, tensors, chunks, chunk,
    act, saved, cot, w_gate, w_up, w_down,
    out_ref, grad_ref,
    gate_buf, up_buf, down_buf, gathered, staging, rows_f32, lhs_two, lhs_cot,
    products, part, arrived, shared, second_f32, total, final_out, final_in,
    load_sem, weight_sem, gather_send, gather_recv, part_send, part_recv,
    share_send, share_recv, final_send, final_recv,
):
    section = lax.axis_index("section")
    outer = lax.axis_index("outer")
    tensor = lax.axis_index("tensor")
    other = lax.rem(section + 1, sections)
    own_rows = act.shape[1]
    rows = own_rows * outers
    cells = own_rows // outers
    shard = rows // tensors

    loads = [
        pltpu.make_async_copy(source.at[0], gathered.at[which, outer], load_sem.at[which])
        for which, source in enumerate((act, saved, cot))
    ]
    for load in loads:
        load.start()

    def weight_copies(c):
        span = pl.ds(pl.multiple_of(c * chunk, chunk), chunk)
        return (
            pltpu.make_async_copy(w_gate.at[0, :, span], gate_buf.at[c], weight_sem.at[0, c]),
            pltpu.make_async_copy(w_up.at[0, :, span], up_buf.at[c], weight_sem.at[1, c]),
            pltpu.make_async_copy(w_down.at[0, span, :], down_buf.at[c], weight_sem.at[2, c]),
        )

    for c in range(min(AHEAD, chunks)):
        for copy in weight_copies(c):
            copy.start(priority=1)

    barrier = pltpu.get_barrier_semaphore()
    for step in range(1, outers):
        pl.semaphore_signal(
            barrier, 1, device_id={"outer": lax.rem(outer + step, outers)}, device_id_type=MESH
        )
    for step in range(1, tensors):
        pl.semaphore_signal(
            barrier, 1, device_id={"tensor": lax.rem(tensor + step, tensors)}, device_id_type=MESH
        )
    for place in range(outers):
        pl.semaphore_signal(
            barrier, 1, device_id={"section": other, "outer": place}, device_id_type=MESH
        )
    pl.semaphore_wait(barrier, 2 * outers + tensors - 2)

    def gather_copy(which, origin, target):
        return pltpu.make_async_remote_copy(
            src_ref=gathered.at[which, origin],
            dst_ref=gathered.at[which, origin],
            send_sem=gather_send.at[which, target],
            recv_sem=gather_recv.at[which, origin],
            device_id={"outer": target},
            device_id_type=MESH,
        )

    for which in range(3):
        loads[which].wait()
        for step in range(1, outers):
            gather_copy(which, outer, lax.rem(outer + step, outers)).start()

    for which in range(3):
        for step in range(1, outers):
            origin = lax.rem(outer + step, outers)
            gather_copy(which, origin, origin).wait_recv()
        for origin in range(outers):
            staging[...] = gathered[which, origin].astype(F32)
            for j in range(outers):
                to = (j * outers + origin) * cells
                rows_f32[which, to : to + cells, :] = staging[j * cells : (j + 1) * cells, :]
    lhs_two[0:rows, :] = rows_f32[0].astype(BF16)
    lhs_two[rows : 2 * rows, :] = rows_f32[1].astype(BF16)
    lhs_cot[...] = rows_f32[2].astype(BF16)
    place = lax.broadcasted_iota(jnp.int32, total.shape[1:], 0)
    mine = lax.rem(lax.div(place, cells), outers) == outer
    total[0] = jnp.where(mine, rows_f32[0], 0.0)
    total[1] = jnp.where(mine, rows_f32[2], 0.0)

    def part_copy(c, origin, target):
        return pltpu.make_async_remote_copy(
            src_ref=part.at[c, target],
            dst_ref=arrived.at[c, origin],
            send_sem=part_send.at[c, target],
            recv_sem=part_recv.at[c, origin],
            device_id={"tensor": target},
            device_id_type=MESH,
        )

    def share_copy(c, origin, target):
        return pltpu.make_async_remote_copy(
            src_ref=shared.at[c, origin],
            dst_ref=shared.at[c, origin],
            send_sem=share_send.at[c, target],
            recv_sem=share_recv.at[c, origin],
            device_id={"tensor": target},
            device_id_type=MESH,
        )

    def first(c):
        @pl.when(c + AHEAD < chunks)
        def _():
            for copy in weight_copies(c + AHEAD):
                copy.start(priority=1)

        for copy in weight_copies(c):
            copy.wait()
        two = lhs_two[...]
        products[0 : 2 * rows, :] = jnp.dot(two, gate_buf[c], preferred_element_type=F32)
        products[2 * rows : 4 * rows, :] = jnp.dot(two, up_buf[c], preferred_element_type=F32)
        products[4 * rows : 5 * rows, :] = lax.dot_general(
            lhs_cot[...], down_buf[c], CONTRACT_LAST, preferred_element_type=F32
        )
        for target in range(tensors):
            for which in range(5):
                part[c, target, which] = products[
                    which * rows + target * shard : which * rows + (target + 1) * shard, :
                ].astype(BF16)
        for step in range(1, tensors):
            part_copy(c, tensor, lax.rem(tensor + step, tensors)).start()

    def combine(c):
        for step in range(1, tensors):
            origin = lax.rem(tensor + step, tensors)
            part_copy(c, origin, origin).wait_recv()
        sums = []
        for which in range(5):
            summed = part[c, tensor, which].astype(F32)
            for step in range(1, tensors):
                summed = summed + arrived[c, lax.rem(tensor + step, tensors), which].astype(F32)
            sums.append(summed)
        gate_pre, gate_saved, up_pre, up_saved, hidden_grad = sums
        squash = jax.nn.sigmoid(gate_saved)
        shared[c, tensor, 0] = (gate_pre * jax.nn.sigmoid(gate_pre) * up_pre).astype(BF16)
        shared[c, tensor, 1] = (
            hidden_grad * up_saved * squash * (1.0 + gate_saved * (1.0 - squash))
        ).astype(BF16)
        shared[c, tensor, 2] = (hidden_grad * gate_saved * squash).astype(BF16)
        for step in range(1, tensors):
            share_copy(c, tensor, lax.rem(tensor + step, tensors)).start()

    def second(c):
        for step in range(1, tensors):
            origin = lax.rem(tensor + step, tensors)
            share_copy(c, origin, origin).wait_recv()
        for origin in range(tensors):
            for which in range(3):
                second_f32[which, origin * shard : (origin + 1) * shard, :] = shared[
                    c, origin, which
                ].astype(F32)
        total[0] += jnp.dot(
            second_f32[0].astype(BF16), down_buf[c], preferred_element_type=F32
        )
        total[1] += lax.dot_general(
            second_f32[1].astype(BF16), gate_buf[c], CONTRACT_LAST, preferred_element_type=F32
        ) + lax.dot_general(
            second_f32[2].astype(BF16), up_buf[c], CONTRACT_LAST, preferred_element_type=F32
        )

    def advance(step, carry):
        @pl.when(step < chunks)
        def _():
            first(step)

        @pl.when((step >= SUM_LAG) & (step < chunks + SUM_LAG))
        def _():
            combine(step - SUM_LAG)

        @pl.when(step >= SECOND_LAG)
        def _():
            second(step - SECOND_LAG)

        return carry

    lax.fori_loop(0, chunks + SECOND_LAG, advance, 0)

    def final_copy(origin, target):
        return pltpu.make_async_remote_copy(
            src_ref=final_out.at[target],
            dst_ref=final_in.at[origin],
            send_sem=final_send.at[target],
            recv_sem=final_recv.at[origin],
            device_id={"section": other, "outer": target},
            device_id_type=MESH,
        )

    for target in range(outers):
        for which in range(2):
            final_out[target, which] = total[
                which, target * own_rows : (target + 1) * own_rows, :
            ].astype(BF16)
        final_copy(outer, target).start()

    def drain(c, carry):
        for step in range(1, tensors):
            target = lax.rem(tensor + step, tensors)
            part_copy(c, tensor, target).wait_send()
            share_copy(c, tensor, target).wait_send()
        return carry

    lax.fori_loop(0, chunks, drain, 0)
    for which in range(3):
        for step in range(1, outers):
            gather_copy(which, outer, lax.rem(outer + step, outers)).wait_send()

    for origin in range(outers):
        final_copy(origin, origin).wait_recv()
    for which, result in enumerate((out_ref, grad_ref)):
        summed = final_in[0, which].astype(F32)
        for origin in range(1, outers):
            summed = summed + final_in[origin, which].astype(F32)
        result[0] = summed.astype(BF16)
    for target in range(outers):
        final_copy(outer, target).wait_send()


def fast_kernel(
    outers, tensors, chunks, chunk, paired,
    act, saved, cot, w_gate, w_up, w_down,
    out_ref,
    gate_buf, up_buf, down_buf, up_turned, gathered, rows_f32, lhs_two, lhs_cot,
    part, arrived, passed, joined, shared, total, final_out, final_in,
    load_sem, weight_sem, gather_send, gather_recv, part_send, part_recv, pass_recv,
    share_send, share_recv, final_send, final_recv,
):
    section = lax.axis_index("section")
    outer = lax.axis_index("outer")
    tensor = lax.axis_index("tensor")
    other = 1 - section
    own_rows = act.shape[1]
    rows = own_rows * outers
    lanes = chunk // 2
    left = tensor < 2
    is_end = (tensor == 0) | (tensor == 3)
    is_inner = jnp.logical_not(is_end)
    inner, end = jnp.where(left, 1, 2), jnp.where(left, 0, 3)
    far_inner, far_end = 3 - inner, 3 - end
    mine_half = jnp.where(left, 0, 1)
    far_half = 1 - mine_half
    peers = [lax.rem(tensor + step, tensors) for step in range(1, tensors)]

    loads = [
        pltpu.make_async_copy(source.at[0], gathered.at[which, outer], load_sem.at[which])
        for which, source in enumerate((act, saved, cot))
    ]
    for load in loads:
        load.start()
    barrier = pltpu.get_barrier_semaphore()
    for step in range(1, outers):
        pl.semaphore_signal(
            barrier, 1, device_id={"outer": lax.rem(outer + step, outers)}, device_id_type=MESH
        )
    for peer in peers:
        pl.semaphore_signal(barrier, 1, device_id={"tensor": peer}, device_id_type=MESH)
    for place in range(outers):
        pl.semaphore_signal(
            barrier, 1, device_id={"section": other, "outer": place}, device_id_type=MESH
        )
    weight_copies = []
    for c in range(chunks):
        span = pl.ds(c * chunk, chunk)
        copies = (
            pltpu.make_async_copy(w_gate.at[0, :, span], gate_buf.at[c], weight_sem.at[0, c]),
            pltpu.make_async_copy(w_up.at[0, :, span], up_buf.at[c], weight_sem.at[1, c]),
            pltpu.make_async_copy(w_down.at[0, span, :], down_buf.at[c], weight_sem.at[2, c]),
        )
        for copy in copies:
            copy.start(priority=1)
        weight_copies.append(copies)

    for load in loads:
        load.wait()
    pl.semaphore_wait(barrier, 2 * outers + tensors - 2)

    def gather_copy(which, origin, target):
        return pltpu.make_async_remote_copy(
            src_ref=gathered.at[which, origin],
            dst_ref=gathered.at[which, origin],
            send_sem=gather_send.at[which, target],
            recv_sem=gather_recv.at[which, origin],
            device_id={"outer": target},
            device_id_type=MESH,
        )

    for which in range(3):
        for step in range(1, outers):
            gather_copy(which, outer, lax.rem(outer + step, outers)).start()
    for which in range(3):
        for step in range(1, outers):
            origin = lax.rem(outer + step, outers)
            gather_copy(which, origin, origin).wait_recv()
        for origin in range(outers):
            rows_f32[which, origin * own_rows : (origin + 1) * own_rows, :] = gathered[
                which, origin
            ].astype(F32)
    row = lax.broadcasted_iota(jnp.int32, (rows, rows), 0)
    column = lax.broadcasted_iota(jnp.int32, (rows, rows), 1)
    takes = lax.rem(row, outers) * own_rows + lax.div(row, outers) == column
    turn = jnp.where(takes, 1.0, 0.0).astype(BF16)
    ordered = [
        jnp.dot(turn, rows_f32[which].astype(BF16), preferred_element_type=F32)
        for which in range(3)
    ]
    lhs_two[0:rows, :] = ordered[0].astype(BF16)
    lhs_two[rows : 2 * rows, :] = ordered[1].astype(BF16)
    lhs_cot[...] = ordered[2].astype(BF16)
    place = lax.broadcasted_iota(jnp.int32, total.shape[1:], 0)
    mine = lax.rem(place, outers) == outer
    total[0] = jnp.where(mine, ordered[0], 0.0)
    total[1] = jnp.where(mine, ordered[2], 0.0)

    def part_copy(c, source, slot, lane, target):
        return pltpu.make_async_remote_copy(
            src_ref=source,
            dst_ref=arrived.at[c, slot],
            send_sem=part_send.at[c, lane],
            recv_sem=part_recv.at[c, slot],
            device_id={"tensor": target},
            device_id_type=MESH,
        )

    def pass_copy(c):
        return pltpu.make_async_remote_copy(
            src_ref=part.at[c, far_half],
            dst_ref=passed.at[c],
            send_sem=part_send.at[c, 0],
            recv_sem=pass_recv.at[c],
            device_id={"tensor": inner},
            device_id_type=MESH,
        )

    def share_copy(c, half, lane, target):
        return pltpu.make_async_remote_copy(
            src_ref=shared.at[c, half],
            dst_ref=shared.at[c, half],
            send_sem=share_send.at[c, lane],
            recv_sem=share_recv.at[c, half],
            device_id={"tensor": target},
            device_id_type=MESH,
        )

    def end_sends(c):
        if c in paired:
            across = pass_copy(c)
        else:
            across = part_copy(c, part.at[c, far_half], 1, 0, far_inner)
        return across, part_copy(c, part.at[c, mine_half], 0, 1, inner)

    def inner_send(c):
        source = joined.at[c] if c in paired else part.at[c, far_half]
        return part_copy(c, source, 2, 0, far_inner)

    def share_sends(c):
        return [
            share_copy(c, mine_half, lane, target)
            for lane, target in enumerate((far_inner, far_end, end))
        ]

    def first(c):
        for copy in weight_copies[c]:
            copy.wait()
        gate = jnp.dot(lhs_two[...], gate_buf[c], preferred_element_type=F32)
        up = jnp.dot(lhs_two[...], up_buf[c], preferred_element_type=F32)
        grad = lax.dot_general(lhs_cot[...], down_buf[c], CONTRACT_LAST, preferred_element_type=F32)
        up_turned[c] = up_buf[c].T
        for half in range(2):
            span = slice(half * lanes, (half + 1) * lanes)
            part[c, half, 0 : 2 * rows] = gate[:, span].astype(BF16)
            part[c, half, 2 * rows : 4 * rows] = up[:, span].astype(BF16)
            part[c, half, 4 * rows : 5 * rows] = grad[:, span].astype(BF16)

        @pl.when(is_end)
        def _():
            for copy in end_sends(c):
                copy.start()

        if c not in paired:
            @pl.when(is_inner)
            def _():
                inner_send(c).start()

    def relay(c):
        @pl.when(is_inner)
        def _():
            pass_copy(c).wait_recv()
            joined[c] = (part[c, far_half].astype(F32) + passed[c].astype(F32)).astype(BF16)
            inner_send(c).start()

    def combine(c):
        @pl.when(is_inner)
        def _():
            slots = (0, 2) if c in paired else (0, 1, 2)
            for slot in slots:
                part_copy(c, part.at[c, 0], slot, 0, inner).wait_recv()
            summed = part[c, mine_half].astype(F32)
            for slot in slots:
                summed = summed + arrived[c, slot].astype(F32)
            gate_pre, gate_saved, up_pre, up_saved, hidden_grad = (
                summed[which * rows : (which + 1) * rows] for which in range(5)
            )
            squash = jax.nn.sigmoid(gate_saved)
            forward = gate_pre * jax.nn.sigmoid(gate_pre) * up_pre
            gate_grad = hidden_grad * up_saved * squash * (1.0 + gate_saved * (1.0 - squash))
            up_grad = hidden_grad * gate_saved * squash
            for which, value in enumerate((forward, gate_grad, up_grad)):
                shared[c, mine_half, which * rows : (which + 1) * rows] = value.astype(BF16)
            for copy in share_sends(c):
                copy.start()

    def final_copy(which, origin, target):
        return pltpu.make_async_remote_copy(
            src_ref=final_out.at[which, target],
            dst_ref=final_in.at[which, origin],
            send_sem=final_send.at[which, target],
            recv_sem=final_recv.at[which, origin],
            device_id={"section": other, "outer": target},
            device_id_type=MESH,
        )

    def send_final(which):
        for target in range(outers):
            final_out[which, target] = total[
                which, target * own_rows : (target + 1) * own_rows, :
            ].astype(BF16)
            final_copy(which, outer, target).start()

    def second(c):
        @pl.when(is_end)
        def _():
            share_copy(c, mine_half, 0, inner).wait_recv()

        share_copy(c, far_half, 0, inner).wait_recv()

        def side(which):
            return jnp.concatenate(
                [shared[c, half, which * rows : (which + 1) * rows] for half in range(2)], axis=1
            )

        total[0] += jnp.dot(side(0), down_buf[c], preferred_element_type=F32)
        if c == chunks - 1:
            send_final(0)
        total[1] += lax.dot_general(
            side(1), gate_buf[c], CONTRACT_LAST, preferred_element_type=F32
        ) + jnp.dot(side(2), up_turned[c], preferred_element_type=F32)

    steps = []
    for c in range(chunks):
        steps.append((c, first, c))
        if c in paired:
            steps.append((c + RELAY_AFTER + 0.1, relay, c))
        steps.append((c + (SUM_AFTER if c in paired else DIRECT_AFTER) + 0.2, combine, c))
        steps.append((c + SECOND_AFTER + 0.3, second, c))
    for _, act_on, c in sorted(steps, key=lambda entry: entry[0]):
        act_on(c)
    send_final(1)

    @pl.when(is_end)
    def _():
        for c in range(chunks):
            for copy in end_sends(c):
                copy.wait_send()

    @pl.when(is_inner)
    def _():
        for c in range(chunks):
            inner_send(c).wait_send()
            for copy in share_sends(c):
                copy.wait_send()

    for which in range(3):
        for step in range(1, outers):
            gather_copy(which, outer, lax.rem(outer + step, outers)).wait_send()
    for which in range(2):
        for origin in range(outers):
            final_copy(which, origin, origin).wait_recv()
        summed = final_in[which, 0].astype(F32)
        for origin in range(1, outers):
            summed = summed + final_in[which, origin].astype(F32)
        out_ref[which] = summed.astype(BF16)
    for which in range(2):
        for target in range(outers):
            final_copy(which, outer, target).wait_send()


def part_out(both, out_ref, grad_ref):
    out_ref[0] = both[0]
    grad_ref[0] = both[1]


def fast_call(outers, tensors, chunk, act_in, saved_in, cotangent, w_gate, w_up, w_down):
    own_rows, model_width = act_in.shape[1:]
    chunks = w_gate.shape[2] // chunk
    rows = own_rows * outers
    lanes = chunk // 2
    dma = pltpu.SemaphoreType.DMA
    both = pl.pallas_call(
        functools.partial(
            fast_kernel, outers, tensors, chunks, chunk, range(DIRECT_FIRST, chunks - DIRECT_LAST)
        ),
        out_shape=jax.ShapeDtypeStruct((2, own_rows, model_width), BF16),
        in_specs=[pl.BlockSpec(memory_space=pl.ANY)] * 6,
        out_specs=pl.BlockSpec(memory_space=pltpu.VMEM),
        scratch_shapes=[
            pltpu.VMEM((chunks, model_width, chunk), BF16),
            pltpu.VMEM((chunks, model_width, chunk), BF16),
            pltpu.VMEM((chunks, chunk, model_width), BF16),
            pltpu.VMEM((chunks, chunk, model_width), BF16),
            pltpu.VMEM((3, outers, own_rows, model_width), BF16),
            pltpu.VMEM((3, rows, model_width), F32),
            pltpu.VMEM((2 * rows, model_width), BF16),
            pltpu.VMEM((rows, model_width), BF16),
            pltpu.VMEM((chunks, 2, 5 * rows, lanes), BF16),
            pltpu.VMEM((chunks, 3, 5 * rows, lanes), BF16),
            pltpu.VMEM((chunks, 5 * rows, lanes), BF16),
            pltpu.VMEM((chunks, 5 * rows, lanes), BF16),
            pltpu.VMEM((chunks, 2, 3 * rows, lanes), BF16),
            pltpu.VMEM((2, rows, model_width), F32),
            pltpu.VMEM((2, outers, own_rows, model_width), BF16),
            pltpu.VMEM((2, outers, own_rows, model_width), BF16),
            dma((3,)),
            dma((3, chunks)),
            dma((3, outers)),
            dma((3, outers)),
            dma((chunks, 2)),
            dma((chunks, 3)),
            dma((chunks,)),
            dma((chunks, 3)),
            dma((chunks, 2)),
            dma((2, outers)),
            dma((2, outers)),
        ],
        compiler_params=pltpu.CompilerParams(
            collective_id=0, has_side_effects=True, vmem_limit_bytes=63 * 1024 * 1024
        ),
    )(act_in, saved_in, cotangent, w_gate, w_up, w_down)
    out = jax.ShapeDtypeStruct((1, own_rows, model_width), BF16)
    return pl.pallas_call(part_out, out_shape=(out, out))(both)


def solution(mesh):
    sections, outers, tensors = (mesh.shape[name] for name in ("section", "outer", "tensor"))

    def on_device(act_in, saved_in, cotangent, w_gate, w_up, w_down):
        own_rows, model_width = act_in.shape[1:]
        width = w_gate.shape[2]
        rows = own_rows * outers
        if sections == 2 and tensors == 4 and own_rows == outers and rows % 16 == 0 and width % 512 == 0:
            if 4 * width * model_width * 2 <= 56 * 1024 * 1024:
                return fast_call(
                    outers, tensors, 512, act_in, saved_in, cotangent, w_gate, w_up, w_down
                )
        shard = rows // tensors
        chunk = next(size for size in (512, 256, 128, width) if width % size == 0)
        chunks = width // chunk
        dma = pltpu.SemaphoreType.DMA
        out = jax.ShapeDtypeStruct((1, own_rows, model_width), BF16)
        return pl.pallas_call(
            functools.partial(kernel, sections, outers, tensors, chunks, chunk),
            out_shape=(out, out),
            in_specs=[pl.BlockSpec(memory_space=pl.ANY)] * 6,
            out_specs=[pl.BlockSpec(memory_space=pltpu.VMEM)] * 2,
            scratch_shapes=[
                pltpu.VMEM((chunks, model_width, chunk), BF16),
                pltpu.VMEM((chunks, model_width, chunk), BF16),
                pltpu.VMEM((chunks, chunk, model_width), BF16),
                pltpu.VMEM((3, outers, own_rows, model_width), BF16),
                pltpu.VMEM((own_rows, model_width), F32),
                pltpu.VMEM((3, rows, model_width), F32),
                pltpu.VMEM((2 * rows, model_width), BF16),
                pltpu.VMEM((rows, model_width), BF16),
                pltpu.VMEM((5 * rows, chunk), F32),
                pltpu.VMEM((chunks, tensors, 5, shard, chunk), BF16),
                pltpu.VMEM((chunks, tensors, 5, shard, chunk), BF16),
                pltpu.VMEM((chunks, tensors, 3, shard, chunk), BF16),
                pltpu.VMEM((3, rows, chunk), F32),
                pltpu.VMEM((2, rows, model_width), F32),
                pltpu.VMEM((outers, 2, own_rows, model_width), BF16),
                pltpu.VMEM((outers, 2, own_rows, model_width), BF16),
                dma((3,)),
                dma((3, chunks)),
                dma((3, outers)),
                dma((3, outers)),
                dma((chunks, tensors)),
                dma((chunks, tensors)),
                dma((chunks, tensors)),
                dma((chunks, tensors)),
                dma((outers,)),
                dma((outers,)),
            ],
            compiler_params=pltpu.CompilerParams(
                collective_id=0, has_side_effects=True, vmem_limit_bytes=60 * 1024 * 1024
            ),
        )(act_in, saved_in, cotangent, w_gate, w_up, w_down)

    return jax.shard_map(
        on_device,
        mesh=mesh,
        in_specs=(
            P("section", "outer", "tensor"),
            P("section", "outer", "tensor"),
            P("section", "outer", "tensor"),
            P("section", "tensor", "outer"),
            P("section", "tensor", "outer"),
            P("section", "outer", "tensor"),
        ),
        out_specs=(P("section", "outer", "tensor"), P("section", "outer", "tensor")),
        check_vma=False,
    )
```

```python
import functools

import jax
import jax.numpy as jnp
from jax import lax
from jax.experimental import pallas as pl
from jax.experimental.pallas import tpu as pltpu
from jax.sharding import PartitionSpec as P

MESH = pl.DeviceIdType.MESH
F32 = jnp.float32
BF16 = jnp.bfloat16
CONTRACT_LAST = (((1,), (1,)), ((), ()))
SUM_LAG = 2
SECOND_LAG = 4
AHEAD = 2
RELAY_AFTER = 2
SUM_AFTER = 4
DIRECT_AFTER = 3
SECOND_AFTER = 6
DIRECT_FIRST = 2
DIRECT_LAST = 0


def kernel(
    sections, outers, tensors, chunks, chunk,
    act, saved, cot, w_gate, w_up, w_down,
    out_ref, grad_ref,
    gate_buf, up_buf, down_buf, gathered, staging, rows_f32, lhs_two, lhs_cot,
    products, part, arrived, shared, second_f32, total, final_out, final_in,
    load_sem, weight_sem, gather_send, gather_recv, part_send, part_recv,
    share_send, share_recv, final_send, final_recv,
):
    section = lax.axis_index("section")
    outer = lax.axis_index("outer")
    tensor = lax.axis_index("tensor")
    other = lax.rem(section + 1, sections)
    own_rows = act.shape[1]
    rows = own_rows * outers
    cells = own_rows // outers
    shard = rows // tensors

    loads = [
        pltpu.make_async_copy(source.at[0], gathered.at[which, outer], load_sem.at[which])
        for which, source in enumerate((act, saved, cot))
    ]
    for load in loads:
        load.start()

    def weight_copies(c):
        span = pl.ds(pl.multiple_of(c * chunk, chunk), chunk)
        return (
            pltpu.make_async_copy(w_gate.at[0, :, span], gate_buf.at[c], weight_sem.at[0, c]),
            pltpu.make_async_copy(w_up.at[0, :, span], up_buf.at[c], weight_sem.at[1, c]),
            pltpu.make_async_copy(w_down.at[0, span, :], down_buf.at[c], weight_sem.at[2, c]),
        )

    for c in range(min(AHEAD, chunks)):
        for copy in weight_copies(c):
            copy.start(priority=1)

    barrier = pltpu.get_barrier_semaphore()
    for step in range(1, outers):
        pl.semaphore_signal(
            barrier, 1, device_id={"outer": lax.rem(outer + step, outers)}, device_id_type=MESH
        )
    for step in range(1, tensors):
        pl.semaphore_signal(
            barrier, 1, device_id={"tensor": lax.rem(tensor + step, tensors)}, device_id_type=MESH
        )
    for place in range(outers):
        pl.semaphore_signal(
            barrier, 1, device_id={"section": other, "outer": place}, device_id_type=MESH
        )
    pl.semaphore_wait(barrier, 2 * outers + tensors - 2)

    def gather_copy(which, origin, target):
        return pltpu.make_async_remote_copy(
            src_ref=gathered.at[which, origin],
            dst_ref=gathered.at[which, origin],
            send_sem=gather_send.at[which, target],
            recv_sem=gather_recv.at[which, origin],
            device_id={"outer": target},
            device_id_type=MESH,
        )

    for which in range(3):
        loads[which].wait()
        for step in range(1, outers):
            gather_copy(which, outer, lax.rem(outer + step, outers)).start()

    for which in range(3):
        for step in range(1, outers):
            origin = lax.rem(outer + step, outers)
            gather_copy(which, origin, origin).wait_recv()
        for origin in range(outers):
            staging[...] = gathered[which, origin].astype(F32)
            for j in range(outers):
                to = (j * outers + origin) * cells
                rows_f32[which, to : to + cells, :] = staging[j * cells : (j + 1) * cells, :]
    lhs_two[0:rows, :] = rows_f32[0].astype(BF16)
    lhs_two[rows : 2 * rows, :] = rows_f32[1].astype(BF16)
    lhs_cot[...] = rows_f32[2].astype(BF16)
    place = lax.broadcasted_iota(jnp.int32, total.shape[1:], 0)
    mine = lax.rem(lax.div(place, cells), outers) == outer
    total[0] = jnp.where(mine, rows_f32[0], 0.0)
    total[1] = jnp.where(mine, rows_f32[2], 0.0)

    def part_copy(c, origin, target):
        return pltpu.make_async_remote_copy(
            src_ref=part.at[c, target],
            dst_ref=arrived.at[c, origin],
            send_sem=part_send.at[c, target],
            recv_sem=part_recv.at[c, origin],
            device_id={"tensor": target},
            device_id_type=MESH,
        )

    def share_copy(c, origin, target):
        return pltpu.make_async_remote_copy(
            src_ref=shared.at[c, origin],
            dst_ref=shared.at[c, origin],
            send_sem=share_send.at[c, target],
            recv_sem=share_recv.at[c, origin],
            device_id={"tensor": target},
            device_id_type=MESH,
        )

    def first(c):
        @pl.when(c + AHEAD < chunks)
        def _():
            for copy in weight_copies(c + AHEAD):
                copy.start(priority=1)

        for copy in weight_copies(c):
            copy.wait()
        two = lhs_two[...]
        products[0 : 2 * rows, :] = jnp.dot(two, gate_buf[c], preferred_element_type=F32)
        products[2 * rows : 4 * rows, :] = jnp.dot(two, up_buf[c], preferred_element_type=F32)
        products[4 * rows : 5 * rows, :] = lax.dot_general(
            lhs_cot[...], down_buf[c], CONTRACT_LAST, preferred_element_type=F32
        )
        for target in range(tensors):
            for which in range(5):
                part[c, target, which] = products[
                    which * rows + target * shard : which * rows + (target + 1) * shard, :
                ].astype(BF16)
        for step in range(1, tensors):
            part_copy(c, tensor, lax.rem(tensor + step, tensors)).start()

    def combine(c):
        for step in range(1, tensors):
            origin = lax.rem(tensor + step, tensors)
            part_copy(c, origin, origin).wait_recv()
        sums = []
        for which in range(5):
            summed = part[c, tensor, which].astype(F32)
            for step in range(1, tensors):
                summed = summed + arrived[c, lax.rem(tensor + step, tensors), which].astype(F32)
            sums.append(summed)
        gate_pre, gate_saved, up_pre, up_saved, hidden_grad = sums
        squash = jax.nn.sigmoid(gate_saved)
        shared[c, tensor, 0] = (gate_pre * jax.nn.sigmoid(gate_pre) * up_pre).astype(BF16)
        shared[c, tensor, 1] = (
            hidden_grad * up_saved * squash * (1.0 + gate_saved * (1.0 - squash))
        ).astype(BF16)
        shared[c, tensor, 2] = (hidden_grad * gate_saved * squash).astype(BF16)
        for step in range(1, tensors):
            share_copy(c, tensor, lax.rem(tensor + step, tensors)).start()

    def second(c):
        for step in range(1, tensors):
            origin = lax.rem(tensor + step, tensors)
            share_copy(c, origin, origin).wait_recv()
        for origin in range(tensors):
            for which in range(3):
                second_f32[which, origin * shard : (origin + 1) * shard, :] = shared[
                    c, origin, which
                ].astype(F32)
        total[0] += jnp.dot(
            second_f32[0].astype(BF16), down_buf[c], preferred_element_type=F32
        )
        total[1] += lax.dot_general(
            second_f32[1].astype(BF16), gate_buf[c], CONTRACT_LAST, preferred_element_type=F32
        ) + lax.dot_general(
            second_f32[2].astype(BF16), up_buf[c], CONTRACT_LAST, preferred_element_type=F32
        )

    def advance(step, carry):
        @pl.when(step < chunks)
        def _():
            first(step)

        @pl.when((step >= SUM_LAG) & (step < chunks + SUM_LAG))
        def _():
            combine(step - SUM_LAG)

        @pl.when(step >= SECOND_LAG)
        def _():
            second(step - SECOND_LAG)

        return carry

    lax.fori_loop(0, chunks + SECOND_LAG, advance, 0)

    def final_copy(origin, target):
        return pltpu.make_async_remote_copy(
            src_ref=final_out.at[target],
            dst_ref=final_in.at[origin],
            send_sem=final_send.at[target],
            recv_sem=final_recv.at[origin],
            device_id={"section": other, "outer": target},
            device_id_type=MESH,
        )

    for target in range(outers):
        for which in range(2):
            final_out[target, which] = total[
                which, target * own_rows : (target + 1) * own_rows, :
            ].astype(BF16)
        final_copy(outer, target).start()

    def drain(c, carry):
        for step in range(1, tensors):
            target = lax.rem(tensor + step, tensors)
            part_copy(c, tensor, target).wait_send()
            share_copy(c, tensor, target).wait_send()
        return carry

    lax.fori_loop(0, chunks, drain, 0)
    for which in range(3):
        for step in range(1, outers):
            gather_copy(which, outer, lax.rem(outer + step, outers)).wait_send()

    for origin in range(outers):
        final_copy(origin, origin).wait_recv()
    for which, result in enumerate((out_ref, grad_ref)):
        summed = final_in[0, which].astype(F32)
        for origin in range(1, outers):
            summed = summed + final_in[origin, which].astype(F32)
        result[0] = summed.astype(BF16)
    for target in range(outers):
        final_copy(outer, target).wait_send()


def fast_kernel(
    outers, tensors, chunks, chunk, paired,
    act, saved, cot, w_gate, w_up, w_down,
    out_ref,
    gate_buf, up_buf, down_buf, up_turned, gathered, rows_f32, lhs_two, lhs_cot,
    part, arrived, passed, joined, shared, total, final_out, final_in, result,
    load_sem, weight_sem, gather_send, gather_recv, part_send, part_recv, pass_recv,
    share_send, share_recv, final_send, final_recv, result_sem,
):
    section = lax.axis_index("section")
    outer = lax.axis_index("outer")
    tensor = lax.axis_index("tensor")
    other = 1 - section
    own_rows = act.shape[1]
    rows = own_rows * outers
    lanes = chunk // 2
    left = tensor < 2
    is_end = (tensor == 0) | (tensor == 3)
    is_inner = jnp.logical_not(is_end)
    inner, end = jnp.where(left, 1, 2), jnp.where(left, 0, 3)
    far_inner, far_end = 3 - inner, 3 - end
    mine_half = jnp.where(left, 0, 1)
    far_half = 1 - mine_half
    peers = [lax.rem(tensor + step, tensors) for step in range(1, tensors)]

    loads = [
        pltpu.make_async_copy(source.at[0], gathered.at[which, outer], load_sem.at[which])
        for which, source in enumerate((act, saved, cot))
    ]
    for load in loads:
        load.start()
    barrier = pltpu.get_barrier_semaphore()
    for step in range(1, outers):
        pl.semaphore_signal(
            barrier, 1, device_id={"outer": lax.rem(outer + step, outers)}, device_id_type=MESH
        )
    for peer in peers:
        pl.semaphore_signal(barrier, 1, device_id={"tensor": peer}, device_id_type=MESH)
    for place in range(outers):
        pl.semaphore_signal(
            barrier, 1, device_id={"section": other, "outer": place}, device_id_type=MESH
        )
    weight_copies = []
    for c in range(chunks):
        span = pl.ds(c * chunk, chunk)
        copies = (
            pltpu.make_async_copy(w_gate.at[0, :, span], gate_buf.at[c], weight_sem.at[0, c]),
            pltpu.make_async_copy(w_up.at[0, :, span], up_buf.at[c], weight_sem.at[1, c]),
            pltpu.make_async_copy(w_down.at[0, span, :], down_buf.at[c], weight_sem.at[2, c]),
        )
        for copy in copies:
            copy.start(priority=1)
        weight_copies.append(copies)

    for load in loads:
        load.wait()
    pl.semaphore_wait(barrier, 2 * outers + tensors - 2)

    def gather_copy(which, origin, target):
        return pltpu.make_async_remote_copy(
            src_ref=gathered.at[which, origin],
            dst_ref=gathered.at[which, origin],
            send_sem=gather_send.at[which, target],
            recv_sem=gather_recv.at[which, origin],
            device_id={"outer": target},
            device_id_type=MESH,
        )

    for which in range(3):
        for step in range(1, outers):
            gather_copy(which, outer, lax.rem(outer + step, outers)).start()
    for which in range(3):
        for step in range(1, outers):
            origin = lax.rem(outer + step, outers)
            gather_copy(which, origin, origin).wait_recv()
        for origin in range(outers):
            rows_f32[which, origin * own_rows : (origin + 1) * own_rows, :] = gathered[
                which, origin
            ].astype(F32)
    row = lax.broadcasted_iota(jnp.int32, (rows, rows), 0)
    column = lax.broadcasted_iota(jnp.int32, (rows, rows), 1)
    takes = lax.rem(row, outers) * own_rows + lax.div(row, outers) == column
    turn = jnp.where(takes, 1.0, 0.0).astype(BF16)
    ordered = [
        jnp.dot(turn, rows_f32[which].astype(BF16), preferred_element_type=F32)
        for which in range(3)
    ]
    lhs_two[0:rows, :] = ordered[0].astype(BF16)
    lhs_two[rows : 2 * rows, :] = ordered[1].astype(BF16)
    lhs_cot[...] = ordered[2].astype(BF16)
    place = lax.broadcasted_iota(jnp.int32, total.shape[1:], 0)
    mine = lax.rem(place, outers) == outer
    total[0] = jnp.where(mine, ordered[0], 0.0)
    total[1] = jnp.where(mine, ordered[2], 0.0)

    def part_copy(c, source, slot, lane, target):
        return pltpu.make_async_remote_copy(
            src_ref=source,
            dst_ref=arrived.at[c, slot],
            send_sem=part_send.at[c, lane],
            recv_sem=part_recv.at[c, slot],
            device_id={"tensor": target},
            device_id_type=MESH,
        )

    def pass_copy(c):
        return pltpu.make_async_remote_copy(
            src_ref=part.at[c, far_half],
            dst_ref=passed.at[c],
            send_sem=part_send.at[c, 0],
            recv_sem=pass_recv.at[c],
            device_id={"tensor": inner},
            device_id_type=MESH,
        )

    def share_copy(c, half, lane, target):
        return pltpu.make_async_remote_copy(
            src_ref=shared.at[c, half],
            dst_ref=shared.at[c, half],
            send_sem=share_send.at[c, lane],
            recv_sem=share_recv.at[c, half],
            device_id={"tensor": target},
            device_id_type=MESH,
        )

    def end_sends(c):
        if c in paired:
            across = pass_copy(c)
        else:
            across = part_copy(c, part.at[c, far_half], 1, 0, far_inner)
        return across, part_copy(c, part.at[c, mine_half], 0, 1, inner)

    def inner_send(c):
        source = joined.at[c] if c in paired else part.at[c, far_half]
        return part_copy(c, source, 2, 0, far_inner)

    def share_sends(c):
        return [
            share_copy(c, mine_half, lane, target)
            for lane, target in enumerate((far_end, far_inner, end))
        ]

    def first(c):
        for copy in weight_copies[c]:
            copy.wait()
        gate = jnp.dot(lhs_two[...], gate_buf[c], preferred_element_type=F32)
        up = jnp.dot(lhs_two[...], up_buf[c], preferred_element_type=F32)
        grad = lax.dot_general(lhs_cot[...], down_buf[c], CONTRACT_LAST, preferred_element_type=F32)
        up_turned[c] = up_buf[c].T
        for half in range(2):
            span = slice(half * lanes, (half + 1) * lanes)
            part[c, half, 0 : 2 * rows] = gate[:, span].astype(BF16)
            part[c, half, 2 * rows : 4 * rows] = up[:, span].astype(BF16)
            part[c, half, 4 * rows : 5 * rows] = grad[:, span].astype(BF16)

        @pl.when(is_end)
        def _():
            for copy in end_sends(c):
                copy.start()

        if c not in paired:
            @pl.when(is_inner)
            def _():
                inner_send(c).start()

    def relay(c):
        @pl.when(is_inner)
        def _():
            pass_copy(c).wait_recv()
            joined[c] = (part[c, far_half].astype(F32) + passed[c].astype(F32)).astype(BF16)
            inner_send(c).start()

    def combine(c):
        @pl.when(is_inner)
        def _():
            slots = (0, 2) if c in paired else (0, 1, 2)
            for slot in slots:
                part_copy(c, part.at[c, 0], slot, 0, inner).wait_recv()
            summed = part[c, mine_half].astype(F32)
            for slot in slots:
                summed = summed + arrived[c, slot].astype(F32)
            gate_pre, gate_saved, up_pre, up_saved, hidden_grad = (
                summed[which * rows : (which + 1) * rows] for which in range(5)
            )
            squash = jax.nn.sigmoid(gate_saved)
            forward = gate_pre * jax.nn.sigmoid(gate_pre) * up_pre
            gate_grad = hidden_grad * up_saved * squash * (1.0 + gate_saved * (1.0 - squash))
            up_grad = hidden_grad * gate_saved * squash
            for which, value in enumerate((forward, gate_grad, up_grad)):
                shared[c, mine_half, which * rows : (which + 1) * rows] = value.astype(BF16)
            for copy in share_sends(c):
                copy.start()

    def final_copy(which, origin, target):
        return pltpu.make_async_remote_copy(
            src_ref=final_out.at[which, target],
            dst_ref=final_in.at[which, origin],
            send_sem=final_send.at[which, target],
            recv_sem=final_recv.at[which, origin],
            device_id={"section": other, "outer": target},
            device_id_type=MESH,
        )

    def result_copy(which):
        return pltpu.make_async_copy(result.at[which], out_ref.at[which], result_sem.at[which])

    def send_final(which):
        for target in range(outers):
            final_out[which, target] = total[
                which, target * own_rows : (target + 1) * own_rows, :
            ].astype(BF16)
            final_copy(which, outer, target).start()

    def second(c):
        @pl.when(is_end)
        def _():
            share_copy(c, mine_half, 0, inner).wait_recv()

        share_copy(c, far_half, 0, inner).wait_recv()

        def side(which):
            return jnp.concatenate(
                [shared[c, half, which * rows : (which + 1) * rows] for half in range(2)], axis=1
            )

        total[0] += jnp.dot(side(0), down_buf[c], preferred_element_type=F32)
        if c == chunks - 1:
            send_final(0)
        total[1] += lax.dot_general(
            side(1), gate_buf[c], CONTRACT_LAST, preferred_element_type=F32
        ) + jnp.dot(side(2), up_turned[c], preferred_element_type=F32)

    steps = []
    for c in range(chunks):
        steps.append((c, first, c))
        if c in paired:
            steps.append((c + RELAY_AFTER + 0.1, relay, c))
        steps.append((c + (SUM_AFTER if c in paired else DIRECT_AFTER) + 0.2, combine, c))
        steps.append((c + SECOND_AFTER + 0.3, second, c))
    for _, act_on, c in sorted(steps, key=lambda entry: entry[0]):
        act_on(c)
    send_final(1)

    @pl.when(is_end)
    def _():
        for c in range(chunks):
            for copy in end_sends(c):
                copy.wait_send()

    @pl.when(is_inner)
    def _():
        for c in range(chunks):
            inner_send(c).wait_send()
            for copy in share_sends(c):
                copy.wait_send()

    for which in range(3):
        for step in range(1, outers):
            gather_copy(which, outer, lax.rem(outer + step, outers)).wait_send()
    for which in range(2):
        for origin in range(outers):
            final_copy(which, origin, origin).wait_recv()
        summed = final_in[which, 0].astype(F32)
        for origin in range(1, outers):
            summed = summed + final_in[which, origin].astype(F32)
        result[which] = summed.astype(BF16)
        result_copy(which).start()
    for which in range(2):
        for target in range(outers):
            final_copy(which, outer, target).wait_send()
        result_copy(which).wait()


def part_out(both, out_ref, grad_ref):
    out_ref[0] = both[0]
    grad_ref[0] = both[1]


def fast_call(outers, tensors, chunk, act_in, saved_in, cotangent, w_gate, w_up, w_down):
    own_rows, model_width = act_in.shape[1:]
    chunks = w_gate.shape[2] // chunk
    rows = own_rows * outers
    lanes = chunk // 2
    dma = pltpu.SemaphoreType.DMA
    both = pl.pallas_call(
        functools.partial(
            fast_kernel, outers, tensors, chunks, chunk, range(DIRECT_FIRST, chunks - DIRECT_LAST)
        ),
        out_shape=jax.ShapeDtypeStruct((2, own_rows, model_width), BF16),
        in_specs=[pl.BlockSpec(memory_space=pl.ANY)] * 6,
        out_specs=pl.BlockSpec(memory_space=pl.ANY),
        scratch_shapes=[
            pltpu.VMEM((chunks, model_width, chunk), BF16),
            pltpu.VMEM((chunks, model_width, chunk), BF16),
            pltpu.VMEM((chunks, chunk, model_width), BF16),
            pltpu.VMEM((chunks, chunk, model_width), BF16),
            pltpu.VMEM((3, outers, own_rows, model_width), BF16),
            pltpu.VMEM((3, rows, model_width), F32),
            pltpu.VMEM((2 * rows, model_width), BF16),
            pltpu.VMEM((rows, model_width), BF16),
            pltpu.VMEM((chunks, 2, 5 * rows, lanes), BF16),
            pltpu.VMEM((chunks, 3, 5 * rows, lanes), BF16),
            pltpu.VMEM((chunks, 5 * rows, lanes), BF16),
            pltpu.VMEM((chunks, 5 * rows, lanes), BF16),
            pltpu.VMEM((chunks, 2, 3 * rows, lanes), BF16),
            pltpu.VMEM((2, rows, model_width), F32),
            pltpu.VMEM((2, outers, own_rows, model_width), BF16),
            pltpu.VMEM((2, outers, own_rows, model_width), BF16),
            pltpu.VMEM((2, own_rows, model_width), BF16),
            dma((3,)),
            dma((3, chunks)),
            dma((3, outers)),
            dma((3, outers)),
            dma((chunks, 2)),
            dma((chunks, 3)),
            dma((chunks,)),
            dma((chunks, 3)),
            dma((chunks, 2)),
            dma((2, outers)),
            dma((2, outers)),
            dma((2,)),
        ],
        compiler_params=pltpu.CompilerParams(
            collective_id=0, has_side_effects=True, vmem_limit_bytes=63 * 1024 * 1024
        ),
    )(act_in, saved_in, cotangent, w_gate, w_up, w_down)
    out = jax.ShapeDtypeStruct((1, own_rows, model_width), BF16)
    return pl.pallas_call(part_out, out_shape=(out, out))(both)


def solution(mesh):
    sections, outers, tensors = (mesh.shape[name] for name in ("section", "outer", "tensor"))

    def on_device(act_in, saved_in, cotangent, w_gate, w_up, w_down):
        own_rows, model_width = act_in.shape[1:]
        width = w_gate.shape[2]
        rows = own_rows * outers
        if sections == 2 and tensors == 4 and own_rows == outers and rows % 16 == 0 and width % 512 == 0:
            if 4 * width * model_width * 2 <= 56 * 1024 * 1024:
                return fast_call(
                    outers, tensors, 512, act_in, saved_in, cotangent, w_gate, w_up, w_down
                )
        shard = rows // tensors
        chunk = next(size for size in (512, 256, 128, width) if width % size == 0)
        chunks = width // chunk
        dma = pltpu.SemaphoreType.DMA
        out = jax.ShapeDtypeStruct((1, own_rows, model_width), BF16)
        return pl.pallas_call(
            functools.partial(kernel, sections, outers, tensors, chunks, chunk),
            out_shape=(out, out),
            in_specs=[pl.BlockSpec(memory_space=pl.ANY)] * 6,
            out_specs=[pl.BlockSpec(memory_space=pltpu.VMEM)] * 2,
            scratch_shapes=[
                pltpu.VMEM((chunks, model_width, chunk), BF16),
                pltpu.VMEM((chunks, model_width, chunk), BF16),
                pltpu.VMEM((chunks, chunk, model_width), BF16),
                pltpu.VMEM((3, outers, own_rows, model_width), BF16),
                pltpu.VMEM((own_rows, model_width), F32),
                pltpu.VMEM((3, rows, model_width), F32),
                pltpu.VMEM((2 * rows, model_width), BF16),
                pltpu.VMEM((rows, model_width), BF16),
                pltpu.VMEM((5 * rows, chunk), F32),
                pltpu.VMEM((chunks, tensors, 5, shard, chunk), BF16),
                pltpu.VMEM((chunks, tensors, 5, shard, chunk), BF16),
                pltpu.VMEM((chunks, tensors, 3, shard, chunk), BF16),
                pltpu.VMEM((3, rows, chunk), F32),
                pltpu.VMEM((2, rows, model_width), F32),
                pltpu.VMEM((outers, 2, own_rows, model_width), BF16),
                pltpu.VMEM((outers, 2, own_rows, model_width), BF16),
                dma((3,)),
                dma((3, chunks)),
                dma((3, outers)),
                dma((3, outers)),
                dma((chunks, tensors)),
                dma((chunks, tensors)),
                dma((chunks, tensors)),
                dma((chunks, tensors)),
                dma((outers,)),
                dma((outers,)),
            ],
            compiler_params=pltpu.CompilerParams(
                collective_id=0, has_side_effects=True, vmem_limit_bytes=60 * 1024 * 1024
            ),
        )(act_in, saved_in, cotangent, w_gate, w_up, w_down)

    return jax.shard_map(
        on_device,
        mesh=mesh,
        in_specs=(
            P("section", "outer", "tensor"),
            P("section", "outer", "tensor"),
            P("section", "outer", "tensor"),
            P("section", "tensor", "outer"),
            P("section", "tensor", "outer"),
            P("section", "outer", "tensor"),
        ),
        out_specs=(P("section", "outer", "tensor"), P("section", "outer", "tensor")),
        check_vma=False,
    )
```
